256 devices in a mesh: rep: 2 (over y), ep: 64 (over z, x), tp: 2 (over core).
Axes of the slice: x: 4, y: 2, z: 16, core: 2. Of those that a mesh axis runs over, the one named last changes fastest.
The devices are a block of a 4x16x16 slice.
Arguments:
- resid: bfloat16 [8192, 1440], P(('rep', 'ep')), parts along dimension 0, may hold values from -6 to 6
- query: bfloat16 [8192, 2048], P(('rep', 'ep'), 'tp'), parts along dimension 0, may hold values from -400 to 400
- key_value_pages: bfloat16 [2, 98304, 16, 256], P(None, ('rep', 'ep'), None, 'tp'), parts along dimension 1, may hold values from -4 to 4
- page_table: int32 [8192, 12], P(('rep', 'ep')), parts along dimension 0, may hold values from 0 to 767, as said below
- ctx_len: int32 [8192], P(('rep', 'ep')), parts along dimension 0, may hold values from 2 to 192, as said below
- experts_chosen: int32 [8192, 4], P(('rep', 'ep')), parts along dimension 0, may hold values from 0 to 63, as said below
- router_logits: float32 [8192, 4], P(('rep', 'ep')), parts along dimension 0, may hold values from -25 to 300
- norm_gain: float32 [1440], replicated, may hold values from 0.25 to 1.75
- out_proj: bfloat16 [2048, 1440], P('tp'), may hold values from -0.125 to 0.125
- w_gate: bfloat16 [64, 1440, 1440], P('ep', None, 'tp'), may hold values from -0.15625 to 0.15625
- w_up: bfloat16 [64, 1440, 1440], P('ep', None, 'tp'), may hold values from -0.15625 to 0.15625
- w_down: bfloat16 [64, 1440, 1440], P('ep', 'tp'), may hold values from -3 to 3
Outputs:
- mixed: bfloat16 [8192, 1440], P(('rep', 'ep'), 'tp'), parts along dimension 0
The draws below stay inside these ranges and needn't reach their ends.
There are 2 independent parts, one for each index of `rep`. The reference program is written for one: setup_inputs(seed, part) draws one part's arguments, and reference() takes and returns one part's arrays. A program takes and returns all parts, laid end to end along the dimension named above; an argument that names none is the same for every part. Nothing has to cross between parts.
Inputs may be any that keep to these rules, and one draw needn't show every extreme that they name: Each block of 64 tokens holds its own pool: the rows of page_table of one block together name each of its 768 pages once. `ctx_len`: every block of 64 tokens has a token with 192 positions. `experts_chosen`: each row names 4 different experts. Within the rows of one device no expert is named by more than 8 rows, and one expert is named by exactly 8 of them.
All inputs are finite; a program needn't handle non-finite values.
Results may differ from the reference program's by a relative error of at most 0.008.
Values may be sent and summed in bfloat16 or wider, within the bound.
A program may use at most 128 MiB of HBM per device.

```python
import math
import jax
import jax.numpy as jnp
from jax import lax

D = 1440
QUERY_HEADS = 32
KEY_VALUE_HEADS = 4
HEAD_WIDTH = 64
FF = 1440
TOP = 4
PAGE_LENGTH = 16
CONTEXT_LIMIT = 192
TOKENS_PER_SHARD = 64
E = 64
TOKEN_COUNT = 4096
CAP = 8
PAGES_TOK = 12
PAGES_PER_SHARD = 768


def table_draw(key):
    blocks = TOKEN_COUNT // TOKENS_PER_SHARD
    subkeys = jax.random.split(jax.random.fold_in(key, 101), blocks)

    def one_pool(subkey):
        return jax.random.permutation(subkey, PAGES_PER_SHARD)
    orders = jax.vmap(one_pool)(subkeys)
    return orders.reshape(TOKEN_COUNT, PAGES_TOK).astype(jnp.int32)


def route_draw(key):
    blocks = TOKEN_COUNT // TOKENS_PER_SHARD
    pairs = TOKENS_PER_SHARD * TOP
    slot_total = E * CAP

    def one_block(subkey):
        parts = jax.random.split(subkey, 5)
        hottest = jax.random.randint(parts[0], (), 0, E, jnp.int32)
        owner = jnp.arange(slot_total, dtype=jnp.int32) // CAP
        favour = jax.random.randint(parts[1], (E,), 0, 3, jnp.int32)
        jitter = jax.random.randint(parts[2], (slot_total,), 0, 65536, jnp.int32)
        priority = jitter + favour[owner] * 32768 + jnp.where(owner == hottest, 1048576, 0).astype(jnp.int32)
        priority = priority * slot_total + jnp.arange(slot_total, dtype=jnp.int32)
        taken = lax.top_k(priority, pairs)[1].astype(jnp.int32)
        ordered = jnp.sort(taken)
        names = (ordered // CAP).reshape(TOP, TOKENS_PER_SHARD).T
        names = names[jax.random.permutation(parts[3], TOKENS_PER_SHARD)]
        column_rank = jax.random.randint(parts[4], (TOKENS_PER_SHARD, TOP), 0, 65536, jnp.int32) * TOP + jnp.arange(TOP, dtype=jnp.int32)[None, :]
        column_order = jnp.argsort(column_rank, axis=1)
        return jnp.take_along_axis(names, column_order, axis=1).astype(jnp.int32)
    subkeys = jax.random.split(jax.random.fold_in(key, 201), blocks)
    return jax.vmap(one_block)(subkeys).reshape(TOKEN_COUNT, TOP).astype(jnp.int32)


def cache_base(key):
    target_shape = (2, TOKEN_COUNT // TOKENS_PER_SHARD * PAGES_PER_SHARD, PAGE_LENGTH, KEY_VALUE_HEADS * HEAD_WIDTH)
    return jax.random.truncated_normal(jax.random.fold_in(key, 104), -4.0, 4.0, target_shape, jnp.float32)


def draw_resid(key, part):
    values = jax.random.truncated_normal(jax.random.fold_in(key, 401), -6.0, 6.0, (TOKEN_COUNT, D), jnp.float32)
    return values.astype(jnp.bfloat16)


def draw_page_table(key, part):
    return table_draw(key)


def draw_ctx_len(key, part):
    blocks = TOKEN_COUNT // TOKENS_PER_SHARD
    lengths = jax.random.randint(jax.random.fold_in(key, 102), (TOKEN_COUNT,), 2, CONTEXT_LIMIT + 1, jnp.int32)
    chosen_row = jax.random.randint(jax.random.fold_in(key, 103), (blocks,), 0, TOKENS_PER_SHARD, jnp.int32)
    marked = jnp.arange(TOKEN_COUNT, dtype=jnp.int32) % TOKENS_PER_SHARD == jnp.repeat(chosen_row, TOKENS_PER_SHARD)
    return jnp.where(marked, CONTEXT_LIMIT, lengths).astype(jnp.int32)


def draw_experts_chosen(key, part):
    return route_draw(key)


def draw_key_value_pages(key, part):
    cache_pages = cache_base(key)
    return cache_pages.astype(jnp.bfloat16)


def draw_query(key, part):
    values = jax.random.truncated_normal(jax.random.fold_in(key, 107), -4.0, 4.0, (TOKEN_COUNT, QUERY_HEADS * HEAD_WIDTH), jnp.float32)
    return values.astype(jnp.bfloat16)


def draw_router_logits(key, part):
    values = jnp.clip(2.0 * jax.random.normal(jax.random.fold_in(key, 109), (TOKEN_COUNT, TOP), jnp.float32), -10.0, 10.0)
    return values


def draw_w_down(key, part):
    values = jax.random.truncated_normal(jax.random.fold_in(key, 301), -4.0, 4.0, (E, FF, D), jnp.float32) / math.sqrt(FF)
    return values.astype(jnp.bfloat16)


def block_scale(own_key, dims, shards, smallest, largest):
    factor_of, own = 1.0, jax.random.fold_in(own_key, 6)
    for position, shards_of in shards:
        heights = jnp.exp(jax.random.uniform(jax.random.fold_in(own, position), (shards_of,), jnp.float32, smallest / len(shards), largest / len(shards)))
        factor_of = factor_of * jnp.repeat(heights, dims[position] // shards_of).reshape([-1 if axis == position else 1 for axis in range(len(dims))])
    return factor_of


def noise(rng, dims, width, reach, cuts=(), kind=jnp.bfloat16):
    drawn = width * jax.random.normal(rng, dims, jnp.float32)
    if cuts:
        drawn = drawn * block_scale(rng, dims, cuts, -0.22, 0.18)
    return jnp.clip(drawn, -reach, reach).astype(kind)


def setup_inputs(seed: int = 0, part: int = 0) -> dict:
    key_of = jax.random.split(jax.random.key(seed), 13)
    own_keys = jax.random.split(jax.random.fold_in(key_of[12], part), 13)
    return {
        "resid": draw_resid(jax.random.fold_in(jax.random.fold_in(key_of[12], part), 71), part),
        "query": draw_query(jax.random.fold_in(jax.random.fold_in(key_of[12], part), 71), part),
        "key_value_pages": draw_key_value_pages(jax.random.fold_in(jax.random.fold_in(key_of[12], part), 71), part),
        "page_table": draw_page_table(jax.random.fold_in(jax.random.fold_in(key_of[12], part), 71), part),
        "ctx_len": draw_ctx_len(jax.random.fold_in(jax.random.fold_in(key_of[12], part), 71), part),
        "experts_chosen": draw_experts_chosen(jax.random.fold_in(jax.random.fold_in(key_of[12], part), 71), part),
        "router_logits": draw_router_logits(jax.random.fold_in(jax.random.fold_in(key_of[12], part), 71), part),
        "norm_gain": jnp.clip(1.0 + 0.15 * jax.random.normal(key_of[7], (D,), jnp.float32), 0.25, 1.75),
        "out_proj": noise(key_of[8], (QUERY_HEADS * HEAD_WIDTH, D), (QUERY_HEADS * HEAD_WIDTH) ** -0.5, 0.125, ((0, 2),)),
        "w_gate": noise(key_of[9], (E, D, FF), D ** -0.5, 0.15625, ((0, 64), (2, 2))),
        "w_up": noise(key_of[10], (E, D, FF), D ** -0.5, 0.15625, ((0, 64), (2, 2))),
        "w_down": draw_w_down(jax.random.fold_in(key_of[12], 71), part),
    }


def reference(resid, query, key_value_pages, page_table, ctx_len, experts_chosen, router_logits, norm_gain, out_proj, w_gate, w_up, w_down):
    blocks = TOKEN_COUNT // TOKENS_PER_SHARD
    group_width = QUERY_HEADS // KEY_VALUE_HEADS

    def attend(index):
        start = index * TOKENS_PER_SHARD
        query_matrix = lax.dynamic_slice_in_dim(query, start, TOKENS_PER_SHARD, 0)
        page_table_rows = lax.dynamic_slice_in_dim(page_table, start, TOKENS_PER_SHARD, 0) + index * PAGES_PER_SHARD
        lengths = lax.dynamic_slice_in_dim(ctx_len, start, TOKENS_PER_SHARD, 0)
        cached_keys = key_value_pages[0][page_table_rows].reshape(TOKENS_PER_SHARD, CONTEXT_LIMIT, KEY_VALUE_HEADS, HEAD_WIDTH).astype(jnp.float32)
        cached_values = key_value_pages[1][page_table_rows].reshape(TOKENS_PER_SHARD, CONTEXT_LIMIT, KEY_VALUE_HEADS, HEAD_WIDTH).astype(jnp.float32)
        query_block = query_matrix.reshape(TOKENS_PER_SHARD, KEY_VALUE_HEADS, group_width, HEAD_WIDTH).astype(jnp.float32)
        scores = jnp.einsum('tgqd,tpgd->tgqp', query_block, cached_keys) * (1.0 / math.sqrt(HEAD_WIDTH))
        visible = jnp.arange(CONTEXT_LIMIT, dtype=jnp.int32)[None, :] < lengths[:, None]
        scores = jnp.where(visible[:, None, None, :], scores, -jnp.inf)
        row_max = lax.optimization_barrier(jnp.max(scores, axis=3, keepdims=True))
        weights = jnp.exp(scores - row_max)
        probability = (weights / lax.optimization_barrier(jnp.sum(weights, axis=3, keepdims=True))).astype(jnp.bfloat16)
        attended = jnp.einsum('tgqp,tpgd->tgqd', probability.astype(jnp.float32), cached_values)
        return attended.astype(jnp.bfloat16).reshape(TOKENS_PER_SHARD, QUERY_HEADS * HEAD_WIDTH)
    attended = lax.map(attend, jnp.arange(blocks, dtype=jnp.int32)).reshape(TOKEN_COUNT, QUERY_HEADS * HEAD_WIDTH)
    stream = resid.astype(jnp.float32) + jnp.dot(attended, out_proj, preferred_element_type=jnp.float32)
    mean_square = lax.optimization_barrier(jnp.mean(stream * stream, axis=1, keepdims=True))
    normed = (stream * lax.rsqrt(mean_square + 1e-05) * norm_gain).astype(jnp.bfloat16)
    gate_weights = jax.nn.softmax(router_logits.astype(jnp.float32), axis=1)
    chosen = experts_chosen.reshape(blocks, TOKENS_PER_SHARD * TOP)
    onehot = (chosen[:, :, None] == jnp.arange(E, dtype=jnp.int32)[None, None, :]).astype(jnp.int32)
    before = jnp.cumsum(onehot, axis=1, dtype=jnp.int32) - onehot
    slot_rank = lax.optimization_barrier(jnp.sum(before * onehot, axis=2, dtype=jnp.int32)).reshape(-1)
    chosen_flat = chosen.reshape(-1)
    source = jnp.repeat(jnp.arange(blocks, dtype=jnp.int32), TOKENS_PER_SHARD * TOP)
    token_rows = jnp.repeat(jnp.arange(TOKEN_COUNT, dtype=jnp.int32), TOP)
    buffer = jnp.zeros((E, blocks, CAP, D), jnp.bfloat16)
    buffer = buffer.at[chosen_flat, source, slot_rank].set(normed[token_rows])

    def expert_apply(operands):
        inputs, gate_matrix, up_matrix, down_matrix = operands
        rows = inputs.reshape(blocks * CAP, D)
        gate_value = jnp.dot(rows, gate_matrix, preferred_element_type=jnp.float32)
        up_value = jnp.dot(rows, up_matrix, preferred_element_type=jnp.float32)
        hidden = (gate_value * jax.nn.sigmoid(1.702 * gate_value) * (up_value + 1.0)).astype(jnp.bfloat16)
        output = jnp.dot(hidden, down_matrix, preferred_element_type=jnp.float32).astype(jnp.bfloat16)
        return output.reshape(blocks, CAP, D)
    outputs = lax.map(expert_apply, (buffer, w_gate, w_up, w_down))
    picked = outputs[chosen_flat, source, slot_rank].astype(jnp.float32).reshape(TOKEN_COUNT, TOP, D)
    expert_mix = lax.optimization_barrier(jnp.sum(picked * gate_weights[:, :, None], axis=1))
    return (stream + expert_mix).astype(jnp.bfloat16)
```

```python
import functools
import math

import jax
import jax.numpy as jnp
from jax import lax
from jax.experimental import pallas as pl
from jax.experimental.pallas import tpu as pltpu
from jax.sharding import PartitionSpec as P

F32, BF16 = jnp.float32, jnp.bfloat16
MESH = pl.DeviceIdType.MESH
HEAD_WIDTH = 64
LANES = 128
UNROLL = 8
ALONG_X = 4
CHUNKS = 4


def up_to(n, m):
    return -(-n // m) * m


def attend_kernel(pt_ref, len_ref, q_ref, kv_ref, o_ref, kv, s_ref, p_ref, sem):
    tokens, rows, lanes = q_ref.shape
    pages = pt_ref.shape[1]
    page = kv_ref.shape[2]
    positions = pages * page
    half = rows // 2
    copies = [pltpu.make_async_copy(kv_ref.at[i], kv.at[i], sem.at[i]) for i in range(2)]
    for copy in copies:
        copy.start()
    copies[0].wait()

    def scores(g, carry):
        for i in range(UNROLL):
            t = g * UNROLL + i
            keys = jnp.concatenate([kv[0, pt_ref[t, j]] for j in range(pages)], axis=0)
            s = lax.dot_general(q_ref[t], keys, (((1,), (1,)), ((), ())), preferred_element_type=F32)
            pos = lax.broadcasted_iota(jnp.int32, (rows, positions), 1)
            s_ref[t] = jnp.where(pos < len_ref[t], s * (1.0 / math.sqrt(HEAD_WIDTH)), -1e30)
        return carry

    lax.fori_loop(0, tokens // UNROLL, scores, 0)

    def soften(g, carry):
        s = s_ref[pl.ds(g * UNROLL, UNROLL)]
        w = jnp.exp(s - jnp.max(s, axis=2, keepdims=True))
        p_ref[pl.ds(g * UNROLL, UNROLL)] = (w / jnp.sum(w, axis=2, keepdims=True)).astype(BF16)
        return carry

    lax.fori_loop(0, tokens // UNROLL, soften, 0)
    copies[1].wait()

    def mix(g, carry):
        for i in range(UNROLL):
            t = g * UNROLL + i
            vals = jnp.concatenate([kv[1, pt_ref[t, j]] for j in range(pages)], axis=0)
            o = jnp.dot(p_ref[t], vals, preferred_element_type=F32)
            lane = lax.broadcasted_iota(jnp.int32, (half, lanes), 1)
            o_ref[pl.ds(pl.multiple_of(t * half, half), half), :] = jnp.where(
                lane < HEAD_WIDTH, o[:half], o[half:]
            )
        return carry

    lax.fori_loop(0, tokens // UNROLL, mix, 0)


def lay_queries(query):
    tokens = query.shape[0]
    q = query.reshape(tokens, 2, -1, HEAD_WIDTH)
    zero = jnp.zeros_like(q[:, 0])
    first = jnp.concatenate([q[:, 0], zero], axis=2)
    return jnp.concatenate([first, jnp.concatenate([zero, q[:, 1]], axis=2)], axis=1)


def attend(query, kv, page_table, ctx_len):
    tokens = query.shape[0]
    laid = lay_queries(query)
    half = laid.shape[1] // 2
    positions = kv.shape[2] * page_table.shape[1]
    vmem = pl.BlockSpec(memory_space=pltpu.VMEM)
    smem = pl.BlockSpec(memory_space=pltpu.SMEM)
    return pl.pallas_call(
        attend_kernel,
        out_shape=jax.ShapeDtypeStruct((tokens * half, 2 * HEAD_WIDTH), F32),
        in_specs=[smem, smem, vmem, pl.BlockSpec(memory_space=pl.ANY)],
        out_specs=vmem,
        scratch_shapes=[
            pltpu.VMEM(kv.shape, BF16),
            pltpu.VMEM((tokens, 2 * half, positions), F32),
            pltpu.VMEM((tokens, 2 * half, positions), BF16),
            pltpu.SemaphoreType.DMA((2,)),
        ],
        name="attend",
    )(page_table, ctx_len, laid, kv)


def layer_kernel(
    cap,
    nz,
    att_ref,
    resid_ref,
    meta_ref,
    gain_ref,
    wo_ref,
    wg_ref,
    wu_ref,
    wd_ref,
    out_ref,
    wo,
    wg,
    wu,
    wd,
    part_s,
    part_r,
    nrm,
    strm,
    agb,
    mb,
    sel,
    xin,
    pin,
    gate_s,
    hid_s,
    ybuf,
    yrec,
    ysend,
    yin,
    ct,
    mix,
    rss,
    rsr,
    w_sem,
    ps_sem,
    pr_sem,
    ag_s,
    ag_r,
    mt_s,
    mt_r,
    x_s,
    x_r,
    p_s,
    p_r,
    y_s,
    y_r,
    b_s,
    b_r,
    rs_s,
    rs_r,
):
    nx = ALONG_X
    far = nz // 2
    tokens, width = resid_ref.shape
    half = out_ref.shape[1]
    wide = agb.shape[3]
    rows = tokens // CHUNKS
    slots = 2 * cap
    e = lax.axis_index("ep")
    t = lax.axis_index("tp")
    z, x = e // nx, lax.rem(e, nx)

    def at(zz, xx, tt):
        return {"ep": zz * nx + xx, "tp": tt}

    right = at(lax.rem(z + 1, nz), x, t)
    left = at(lax.rem(z + nz - 1, nz), x, t)
    ahead = (right, left)
    partner = at(z, x, 1 - t)
    plus = [None] + [at(z, lax.rem(x + j, nx), t) for j in range(1, nx)]
    minus = [None] + [at(z, lax.rem(x + nx - j, nx), t) for j in range(1, nx)]

    barrier = pltpu.get_barrier_semaphore()
    for d in (right, left, partner, *plus[1:]):
        pl.semaphore_signal(barrier, inc=1, device_id=d, device_id_type=MESH)

    def remote(src, dst, ss, rs, dev):
        return pltpu.make_async_remote_copy(
            src_ref=src, dst_ref=dst, send_sem=ss, recv_sem=rs, device_id=dev, device_id_type=MESH
        )

    pairs = wo_ref.shape[0] // (2 * HEAD_WIDTH)
    loads = []
    for p in range(pairs):
        for g in range(2):
            loads.append(
                pltpu.make_async_copy(
                    wo_ref.at[pl.ds((g * pairs + p) * HEAD_WIDTH, HEAD_WIDTH)],
                    wo.at[pl.ds((2 * p + g) * HEAD_WIDTH, HEAD_WIDTH)],
                    w_sem.at[2 * p + g],
                )
            )
    n = 2 * pairs
    w_loads = [
        pltpu.make_async_copy(wg_ref, wg.at[pl.ds(0, width)], w_sem.at[n]),
        pltpu.make_async_copy(wu_ref, wu.at[pl.ds(0, width)], w_sem.at[n + 1]),
        pltpu.make_async_copy(wd_ref, wd, w_sem.at[n + 2]),
    ]
    for c in loads + w_loads:
        c.start()
    pad = wg.shape[0] - width
    wg[pl.ds(width, pad), :] = jnp.zeros((pad, wg.shape[1]), BF16)
    wu[pl.ds(width, pad), :] = jnp.zeros((pad, wu.shape[1]), BF16)

    acc = None
    for q in range(0, pairs, 2):
        for c in loads[2 * q : 2 * q + 4]:
            c.wait()
        a = jnp.concatenate(
            [att_ref[pl.ds(p, tokens, stride=pairs), :].astype(BF16) for p in (q, q + 1)], axis=1
        )
        term = jnp.dot(a, wo[pl.ds(q * LANES, 2 * LANES), :], preferred_element_type=F32)
        part_s[:, :width] = term if q == 0 else part_s[:, :width] + term
    fill = part_s.shape[1] - width
    part_s[:, width:] = jnp.zeros((tokens, fill), F32)

    pl.semaphore_wait(barrier, 2 + nx)
    swap = remote(part_s, part_r, ps_sem, pr_sem, partner)
    swap.start()

    mb[0, 0] = meta_ref[0]
    mb[far, 1] = meta_ref[1]
    lane = lax.broadcasted_iota(jnp.int32, (2 * cap, LANES), 1)
    sub = lax.broadcasted_iota(jnp.int32, (2 * cap, LANES), 0)
    r_i = lax.broadcasted_iota(jnp.int32, (LANES, LANES), 0)
    c_i = lax.broadcasted_iota(jnp.int32, (LANES, LANES), 1)
    same = (r_i < tokens) == (c_i < tokens)
    earlier = jnp.where((r_i < c_i) & same, 1.0, 0.0).astype(BF16)

    def ag_copy(s, d, c):
        src = agb.at[far, 1, pl.ds(c * rows, rows)] if s == 1 else agb.at[s - 1, d, pl.ds(c * rows, rows)]
        dst = agb.at[far, 0, pl.ds(c * rows, rows)] if s == far else agb.at[s, d, pl.ds(c * rows, rows)]
        return remote(src, dst, ag_s.at[s, d, c], ag_r.at[s, d, c], ahead[d])

    def mt_copy(s, d):
        src = (mb.at[0, 0] if d == 0 else mb.at[far, 1]) if s == 1 else mb.at[s - 1, d]
        return remote(src, mb.at[s, d], mt_s.at[s, d], mt_r.at[s, d], ahead[d])

    def travels(s, d, c):
        return s < far or (c < CHUNKS // 2) == (d == 0)

    def meta_travels(s, d):
        return s < far or d == 0

    sent = []

    def go(copy):
        copy.start()
        sent.append(copy)

    for d in range(2):
        go(mt_copy(1, d))
    swap.wait_recv()
    for c in range(CHUNKS):
        at_rows = pl.ds(c * rows, rows)
        total = part_s[at_rows, :] + part_r[at_rows, :]
        stream = total[:, :width] + resid_ref[at_rows, :].astype(F32)
        ms = jnp.sum(stream * stream, axis=1, keepdims=True) / width
        normed = (stream * lax.rsqrt(ms + 1e-05) * gain_ref[...]).astype(BF16)
        nrm[0, at_rows, :] = normed[:, :wide]
        nrm[1, at_rows, : width - wide] = normed[:, wide:]
        nrm[1, at_rows, width - wide :] = jnp.zeros((rows, 2 * wide - width), BF16)
        strm[at_rows, :width] = stream
        agb[far, 1, at_rows, :] = nrm[t, at_rows, :]
        for d in range(2):
            go(ag_copy(1, d, c))
    swap.wait_send()

    def halves(ref, at_rows):
        v = ref[at_rows, :]
        return v[:, :wide], pltpu.roll(v, v.shape[1] - half, 1)[:, :wide]

    def select(g):
        m = jnp.where(lane[:8] < tokens, mb[g, 0], mb[g, 1])
        chosen, gates = m[:4], m[4:]
        named, weight = [], []
        for j in range(nx):
            own = (z * nx + lax.rem(x + j, nx)).astype(F32)
            hit = chosen == own
            named.append(jnp.sum(jnp.where(hit, 1.0, 0.0), axis=0, keepdims=True))
            weight.append(jnp.sum(jnp.where(hit, gates, 0.0), axis=0, keepdims=True))
        a = jnp.concatenate(named + named, axis=0)
        rank = jnp.dot(a.astype(BF16), earlier, preferred_element_type=F32)
        blocks = []
        for j in range(nx):
            right_slot = rank[j : j + 1] == lax.rem(sub, cap).astype(F32)
            right_side = (sub < cap) == (lane < tokens)
            block = jnp.where(right_slot & right_side & (named[j] > 0.5), 1.0, 0.0)
            blocks.append(block)
            ct[g - 1, pl.ds(j * slots, slots), :] = block * weight[j]
        place = jnp.concatenate(blocks, axis=0).astype(BF16)
        rows_in = jnp.concatenate([agb[g, 0], agb[g, 1]], axis=0)
        picked = jnp.dot(place, rows_in, preferred_element_type=F32).astype(BF16)
        xin[g, 0] = picked[:slots]
        for j in range(1, nx):
            sel[g, j] = picked[j * slots : (j + 1) * slots]
            go(remote(sel.at[g, j], xin.at[g, j], x_s.at[g, j], x_r.at[g, j], plus[j]))

    def pass_on(g):
        for j in range(1, nx):
            remote(sel.at[g, j], xin.at[g, j], x_s.at[g, j], x_r.at[g, j], plus[j]).wait_recv()
        go(remote(xin.at[g], pin.at[g], p_s.at[g], p_r.at[g], partner))

    def both(g, w):
        lhs0 = xin[g].reshape(nx * slots, wide)
        lhs1 = pin[g].reshape(nx * slots, wide)
        own = pl.ds(pl.multiple_of(t * wide, wide), wide)
        other = pl.ds(pl.multiple_of((1 - t) * wide, wide), wide)
        return jnp.dot(lhs0, w[own, :], preferred_element_type=F32) + jnp.dot(
            lhs1, w[other, :], preferred_element_type=F32
        )

    def gate_up_a(g):
        if g == 1:
            for c in w_loads:
                c.wait()
        remote(xin.at[g], pin.at[g], p_s.at[g], p_r.at[g], partner).wait_recv()
        gate_s[...] = both(g, wg)

    def gate_up_b(g):
        up = both(g, wu)
        gate = gate_s[...]
        hid_s[...] = (gate * jax.nn.sigmoid(1.702 * gate) * (up + 1.0)).astype(BF16)

    def down_a(g):
        ybuf[g, 0] = jnp.dot(hid_s[...], wd[:, :wide], preferred_element_type=F32)

    def down_b(g):
        m = nx * slots
        hi = jnp.dot(hid_s[...], wd[:, wide:], preferred_element_type=F32)
        for r in range(0, m, 16):
            lo = ybuf[g, 0, pl.ds(r, 16), :]
            v = jnp.concatenate([lo, hi[r : r + 16], jnp.zeros((16, 2 * wide - width), F32)], axis=1)
            ybuf[g, 1, pl.ds(r, 16), :] = pltpu.roll(v, 2 * wide - half, 1)[:, :wide]
        go(remote(ybuf.at[g, 1 - t], yrec.at[g], y_s.at[g], y_r.at[g], partner))

    def send_back(g):
        remote(ybuf.at[g, 1 - t], yrec.at[g], y_s.at[g], y_r.at[g], partner).wait_recv()
        y = (ybuf[g, t] + yrec[g]).astype(BF16)
        yin[g, 0] = y[:slots]
        for j in range(1, nx):
            ysend[g, j] = y[j * slots : (j + 1) * slots]
            go(remote(ysend.at[g, j], yin.at[g, j], b_s.at[g, j], b_r.at[g, j], minus[j]))

    def combine(g):
        for j in range(1, nx):
            remote(ysend.at[g, j], yin.at[g, j], b_s.at[g, j], b_r.at[g, j], minus[j]).wait_recv()
        c = ct[g - 1].T
        hi = c.astype(BF16)
        lo = (c - hi.astype(F32)).astype(BF16)
        y = yin[g].reshape(nx * slots, wide)
        mix[g - 1] = jnp.dot(hi, y, preferred_element_type=F32) + jnp.dot(lo, y, preferred_element_type=F32)

    plan = {
        0: ((pass_on, 2), (down_a, 3), (send_back, 4)),
        1: ((down_b, 3),),
        2: ((gate_up_a, 2), (combine, 5)),
        3: ((gate_up_b, 2), (select, 0)),
    }
    for s in range(1, 2 * far + 1):
        if s <= far:
            for d in range(2):
                if meta_travels(s, d):
                    mt_copy(s, d).wait_recv()
                    if s < far and meta_travels(s + 1, d):
                        go(mt_copy(s + 1, d))
        for c in range(CHUNKS):
            if s <= far:
                for d in range(2):
                    cc = c if d == 0 or s < far else CHUNKS - 1 - c
                    if travels(s, d, cc):
                        ag_copy(s, d, cc).wait_recv()
                        if s < far and travels(s + 1, d, cc):
                            go(ag_copy(s + 1, d, cc))
            for stage, lag in plan[c]:
                if 1 <= s - lag <= far:
                    stage(s - lag)

    def rs_copy(k, d, c):
        return remote(
            rss.at[k, d, pl.ds(c * rows, rows)],
            rsr.at[k - 1, d, pl.ds(c * rows, rows)],
            rs_s.at[k, d, c],
            rs_r.at[k, d, c],
            ahead[1 - d],
        )

    def give(k, d, c):
        at_rows = pl.ds(c * rows, rows)
        own_rows = pl.ds((0 if k == far else d * tokens) + c * rows, rows)
        v = mix[k - 1, own_rows, :]
        if k < far and travels(k + 1, d, c):
            rs_copy(k + 1, d, c).wait_recv()
            v = v + rsr[k, d, at_rows, :].astype(F32)
        rss[k, d, at_rows, :] = v.astype(BF16)
        go(rs_copy(k, d, c))

    for k in range(far, 0, -1):
        for c in range(CHUNKS):
            for d in range(2):
                cc = c if d else (c + CHUNKS // 2) % CHUNKS
                if travels(k, d, cc):
                    give(k, d, cc)
    for c in range(CHUNKS):
        cc = (c + CHUNKS // 2) % CHUNKS
        at_rows = pl.ds(cc * rows, rows)
        lo, hi = halves(strm, at_rows)
        stream = jnp.where(t == 0, lo, hi)
        v = stream + mix[far - 1, pl.ds(tokens + cc * rows, rows), :]
        for d in range(2):
            rs_copy(1, d, cc).wait_recv()
            v = v + rsr[0, d, at_rows, :].astype(F32)
        out_ref[at_rows, :] = v[:, :half].astype(BF16)
    for copy in sent:
        copy.wait_send()


def rest(att, resid, meta, gain, out_proj, w_gate, w_up, w_down, cap, nz):
    tokens, width = resid.shape
    half = width // 2
    wide = up_to(half, LANES)
    far = nz // 2
    slots = 2 * cap
    hidden = w_gate.shape[1]
    vmem = pl.BlockSpec(memory_space=pltpu.VMEM)
    hbm = pl.BlockSpec(memory_space=pl.ANY)
    V, S = pltpu.VMEM, pltpu.SemaphoreType.DMA
    g1 = far + 1
    scratch = [
        V(out_proj.shape, BF16),
        V((2 * wide, hidden), BF16),
        V((2 * wide, hidden), BF16),
        V(w_down.shape, BF16),
        V((tokens, 2 * wide), F32),
        V((tokens, 2 * wide), F32),
        V((2, tokens, wide), BF16),
        V((tokens, 2 * wide), F32),
        V((g1, 2, tokens, wide), BF16),
        V((g1, 2, 8, LANES), F32),
        V((g1, ALONG_X, slots, wide), BF16),
        V((g1, ALONG_X, slots, wide), BF16),
        V((g1, ALONG_X, slots, wide), BF16),
        V((ALONG_X * slots, hidden), F32),
        V((ALONG_X * slots, hidden), BF16),
        V((g1, 2, ALONG_X * slots, wide), F32),
        V((g1, ALONG_X * slots, wide), F32),
        V((g1, ALONG_X, slots, wide), BF16),
        V((g1, ALONG_X, slots, wide), BF16),
        V((far, ALONG_X * slots, LANES), F32),
        V((far, 2 * tokens, wide), F32),
        V((g1, 2, tokens, wide), BF16),
        V((g1, 2, tokens, wide), BF16),
        S((2 * (out_proj.shape[0] // (2 * HEAD_WIDTH)) + 3,)),
        S,
        S,
        S((g1, 2, CHUNKS)),
        S((g1, 2, CHUNKS)),
        S((g1, 2)),
        S((g1, 2)),
        S((g1, ALONG_X)),
        S((g1, ALONG_X)),
        S((g1,)),
        S((g1,)),
        S((g1,)),
        S((g1,)),
        S((g1, ALONG_X)),
        S((g1, ALONG_X)),
        S((g1, 2, CHUNKS)),
        S((g1, 2, CHUNKS)),
    ]
    return pl.pallas_call(
        functools.partial(layer_kernel, cap, nz),
        out_shape=jax.ShapeDtypeStruct((tokens, half), BF16),
        in_specs=[vmem] * 4 + [hbm] * 4,
        out_specs=vmem,
        scratch_shapes=scratch,
        compiler_params=pltpu.CompilerParams(collective_id=0, has_side_effects=True, vmem_limit_bytes=56 << 20),
        name="layer",
    )(att, resid, meta, gain, out_proj, w_gate, w_up, w_down)


def body(
    resid,
    query,
    key_value_pages,
    page_table,
    ctx_len,
    experts_chosen,
    router_logits,
    norm_gain,
    out_proj,
    w_gate,
    w_up,
    w_down,
):
    tokens, top = experts_chosen.shape
    owners = lax.axis_size("ep")
    experts = w_gate.shape[0] * owners
    cap = max(2, min(tokens, 2 * tokens * top // experts))
    att = attend(query, key_value_pages, page_table, ctx_len)
    gates = jax.nn.softmax(router_logits, axis=1)
    empty = jnp.full((top, LANES - tokens), -1.0, F32)
    chosen_t = experts_chosen.T.astype(F32)
    none = jnp.zeros((top, LANES - tokens), F32)
    meta = jnp.stack(
        [
            jnp.concatenate([jnp.concatenate([chosen_t, empty], 1), jnp.concatenate([gates.T, none], 1)], 0),
            jnp.concatenate([jnp.concatenate([empty, chosen_t], 1), jnp.concatenate([none, gates.T], 1)], 0),
        ]
    )
    return rest(
        att, resid, meta, norm_gain[None], out_proj, w_gate[0], w_up[0], w_down[0], cap, owners // ALONG_X
    )


def solution(mesh):
    return jax.shard_map(
        body,
        mesh=mesh,
        in_specs=(
            P(("rep", "ep"), None),
            P(("rep", "ep"), "tp"),
            P(None, ("rep", "ep"), None, "tp"),
            P(("rep", "ep"), None),
            P(("rep", "ep")),
            P(("rep", "ep"), None),
            P(("rep", "ep"), None),
            P(),
            P("tp", None),
            P("ep", None, "tp"),
            P("ep", None, "tp"),
            P("ep", "tp", None),
        ),
        out_specs=P(("rep", "ep"), "tp"),
        check_vma=False,
    )
```
